64 devices in a mesh: dp: 4 (over x, y), sp: 16 (over z, core).
Axes of the slice: x: 2, y: 2, z: 8, core: 2. Of those that a mesh axis runs over, the one named last changes fastest.
The devices are a block of a 4x4x8 slice.
Arguments:
- x: bfloat16 [32768, 2304], P(('dp', 'sp')), parts along dimension 0
- gain: bfloat16 [2304], replicated
- wq: bfloat16 [2304, 2048], P('sp')
- wk: bfloat16 [2304, 1024], P('sp')
- wv: bfloat16 [2304, 1024], P('sp')
- wo: bfloat16 [2048, 2304], P('sp')
Outputs:
- output: bfloat16 [32768, 2304], P(('dp', 'sp')), parts along dimension 0
There are 4 independent parts. The reference program is written for one: setup_inputs(seed, part) draws one part's arguments, and reference() takes and returns one part's arrays. A program takes and returns all parts, laid end to end along the dimension named above; an argument that names none is the same for every part.
All inputs are finite; a program needn't handle non-finite values.
Results may differ from the reference program's by a relative error of at most 0.012.
Values are sent between devices in bfloat16 or wider.
A program may use at most 768 MiB of HBM per device.

```python
import jax
import jax.numpy as jnp
from jax import lax

ROWS = 8192
D = 2304
HEADS = 8
KV_HEADS = 4
HEAD = 256
THETA = 10000


def setup_inputs(seed: int = 0, part: int = 0) -> dict:
    kx, kn, kq, kk, kv, ko = jax.random.split(jax.random.key(seed), 6)

    def weights(key, rows, columns):
        return jax.random.normal(key, (rows, columns), jnp.float32) * rows**-0.5

    drawn = {
        "x": jax.random.normal(jax.random.fold_in(kx, part), (ROWS, D), jnp.float32),
        "gain": 1 + 0.1 * jax.random.normal(kn, (D,), jnp.float32),
        "wq": 2 * weights(kq, D, HEADS * HEAD),
        "wk": 2 * weights(kk, D, KV_HEADS * HEAD),
        "wv": 4 * weights(kv, D, KV_HEADS * HEAD),
        "wo": weights(ko, HEADS * HEAD, D),
    }
    return {k: v.astype(jnp.bfloat16) for k, v in drawn.items()}


def normed(x, gain):
    wide = x.astype(jnp.float32)
    scale = lax.rsqrt(jnp.mean(wide * wide, -1, keepdims=True) + 1e-6)
    return (wide * scale * gain.astype(jnp.float32)).astype(jnp.bfloat16)


def turned(t, place, theta):
    half = t.shape[-1] // 2
    angle = place.astype(jnp.float32)[:, None] * theta ** (-jnp.arange(half, dtype=jnp.float32) / half)
    cos, sin = jnp.cos(angle)[:, None], jnp.sin(angle)[:, None]
    a, b = t[..., :half].astype(jnp.float32), t[..., half:].astype(jnp.float32)
    return jnp.concatenate([a * cos - b * sin, b * cos + a * sin], -1).astype(jnp.bfloat16)


def matmul(a, w):
    return jnp.dot(a, w, preferred_element_type=jnp.float32).astype(jnp.bfloat16)


def einsum(form, a, b):
    return jnp.einsum(form, a.astype(jnp.float32), b.astype(jnp.float32))


def attention(q, k, v):
    scores = einsum("tgsd,ugd->gstu", q, k) * q.shape[-1] ** -0.5
    token = jnp.arange(q.shape[0])
    scores = jnp.where(token[:, None] >= token, scores, -jnp.inf)
    weights = jax.nn.softmax(scores, -1).astype(jnp.bfloat16)
    return einsum("gstu,ugd->tgsd", weights, v).astype(jnp.bfloat16)


def reference(x, gain, wq, wk, wv, wo):
    a, place = normed(x, gain), jnp.arange(ROWS)
    q = turned(matmul(a, wq).reshape(ROWS, HEADS, HEAD), place, THETA).reshape(ROWS, KV_HEADS, -1, HEAD)
    k = turned(matmul(a, wk).reshape(ROWS, KV_HEADS, HEAD), place, THETA)
    v = matmul(a, wv).reshape(ROWS, KV_HEADS, HEAD)
    seen = attention(q, k, v).reshape(ROWS, HEADS * HEAD)
    return (x.astype(jnp.float32) + jnp.dot(seen, wo, preferred_element_type=jnp.float32)).astype(jnp.bfloat16)
```

```python
import functools
import math

import jax
import jax.numpy as jnp
from jax import lax
from jax.experimental import pallas as pl
from jax.experimental.pallas import tpu as pltpu
from jax.sharding import PartitionSpec as P

HEAD = 256
THETA = 10000
KVH = 2
GROUP = 2
NEG = -1e30
HIDDEN = 2 * NEG
LOG2E = 1.4426950408889634
BK = 512
STRIP = 512
MESH = pl.DeviceIdType.MESH
F32, BF16 = jnp.float32, jnp.bfloat16


def _dot(a, b, ca, cb):
    return lax.dot_general(a, b, (((ca,), (cb,)), ((), ())), preferred_element_type=F32)


def _at(i, unit):
    return pl.multiple_of(i * unit, unit) if not isinstance(i, int) else i * unit


def kernel(dp, sp, x_ref, gain_ref, cos_ref, sin_ref, wq_ref, wk_ref, wv_ref, wo_ref, y_ref,
           a_s, xr_s, wa_s, wqf_s, wof_s, kv_s, q_s, top_s, mix_s, o_s, os_s,
           x_sem, pre_sem, pre_send, zr_sem, zs_sem, xyr_sem, xys_sem, kr_sem, ks_sem, o_sem, wo_sem):
    g, me = lax.axis_index("dp"), lax.axis_index("sp")
    n = sp // 2
    c, k = lax.div(me, 2), lax.rem(me, 2)
    sib = (g, 2 * c + 1 - k)
    right = (g, 2 * lax.rem(c + 1, n) + k)
    left = (g, 2 * lax.rem(c + n - 1, n) + k)
    own, d = x_ref.shape
    rows, rows_o = wq_ref.shape[0], wo_ref.shape[0]
    tokens = 2 * own
    half = wa_s.shape[1]
    up, down = n // 2, (n - 1) // 2

    def remote(src, dst, ssem, rsem, dev):
        return pltpu.make_async_remote_copy(src_ref=src, dst_ref=dst, send_sem=ssem, recv_sem=rsem, device_id=dev, device_id_type=MESH)

    barrier = pltpu.get_barrier_semaphore()
    for dev in (sib, left, right):
        pl.semaphore_signal(barrier, inc=1, device_id=dev, device_id_type=MESH)

    def greet(p, _):
        pl.semaphore_signal(barrier, inc=1, device_id=(lax.rem(g + p, dp), me), device_id_type=MESH)

    lax.fori_loop(1, dp, greet, None)
    pl.semaphore_wait(barrier, 3 + dp - 1)

    r, b = lax.div(g, dp // 2), lax.rem(g, dp // 2)
    wide = 2 * half // dp
    sub = min(wide, half // 2)
    hi, ho = rows_o // (dp // 2), d // 2

    def piece(mat, o):
        if mat < 2:
            return (wa_s, wqf_s)[mat].at[pl.ds(pl.multiple_of((2 * o + r) * rows, 16), rows), pl.ds(pl.multiple_of(b * wide, 128), wide)]
        return wof_s.at[pl.ds(pl.multiple_of((2 * o + k) * rows_o + b * hi, 16), hi), pl.ds(pl.multiple_of(r * ho, 128), ho)]

    def sources(mat, kk, i):
        at = b * wide + i * sub
        if mat == 1:
            return [(None, wq_ref.at[:, pl.ds(pl.multiple_of(kk * half + at, 128), sub)])]
        h2 = half // 2
        return [(at < h2, wk_ref.at[:, pl.ds(pl.multiple_of(kk * h2 + lax.rem(at, h2), 128), sub)]),
                (at >= h2, wv_ref.at[:, pl.ds(pl.multiple_of(kk * h2 + lax.rem(at, h2), 128), sub)])]

    def maybe(cond, f):
        f() if cond is None else pl.when(cond)(f)

    def begin(mat):
        if mat == 2:
            src = wo_ref.at[pl.ds(pl.multiple_of(b * hi, 16), hi), pl.ds(pl.multiple_of(r * ho, 128), ho)]
            pltpu.make_async_copy(src, piece(2, c), pre_sem.at[2]).start()
            return

        @pl.when(k == r)
        def _():
            for i in range(wide // sub):
                for cond, src in sources(mat, k, i):
                    maybe(cond, lambda: pltpu.make_async_copy(src, piece(mat, c).at[:, pl.ds(i * sub, sub)], pre_sem.at[mat]).start())
                for cond, src in sources(mat, 1 - k, i):
                    maybe(cond, lambda: remote(src, piece(mat, c).at[:, pl.ds(i * sub, sub)], pre_send.at[mat], pre_sem.at[mat], sib).start())

    def begun(mat):
        pltpu.make_async_copy(piece(mat, c), piece(mat, c), pre_sem.at[mat]).wait()

    def hop(mat, o, way, step):
        remote(piece(mat, o), piece(mat, o), zs_sem.at[mat], zr_sem.at[mat, way, step], (right, left)[way]).start()

    def across(mat, o):
        def send(p, _):
            remote(piece(mat, o), piece(mat, o), xys_sem.at[mat], xyr_sem.at[mat], (lax.rem(g + p, dp), me)).start()

        lax.fori_loop(1, dp, send, None)

    def ring(mat, now):
        for s in range(1, up + 1):
            for way, last in ((0, up), (1, down)):
                if s <= last:
                    o = lax.rem(c + n - s, n) if way == 0 else lax.rem(c + s, n)
                    pltpu.make_async_copy(piece(mat, o), piece(mat, o), zr_sem.at[mat, way, s - 1]).wait()
                    if s < last:
                        hop(mat, o, way, s)
                    if now:
                        across(mat, o)

    def across_all(mat):
        lax.fori_loop(0, n, lambda o, _: across(mat, o), None)

    def bytes_of(mat):
        if mat < 2:
            return (wa_s, wqf_s)[mat].at[pl.ds(0, n * 2 * rows * (dp - 1) // dp), :]
        return wof_s.at[pl.ds(0, n * rows_o * (dp - 1) // dp), :]

    def arrived(mat):
        pltpu.make_async_copy(bytes_of(mat), bytes_of(mat), xyr_sem.at[mat]).wait()

    mine = pl.ds(pl.multiple_of(k * own, own), own)
    other = pl.ds(pl.multiple_of((1 - k) * own, own), own)
    begin(0)
    x_in = pltpu.make_async_copy(x_ref, xr_s, x_sem.at[0])
    x_in.start()
    x_out = remote(x_ref, a_s.at[mine, :], x_sem.at[1], x_sem.at[2], sib)
    x_out.start()
    begin(1)
    begin(2)
    for mat in range(3):
        begun(mat)
        if up:
            hop(mat, c, 0, 0)
        if down:
            hop(mat, c, 1, 0)
        if mat == 0:
            across(0, c)
    x_in.wait()

    gain = gain_ref[...].astype(F32)
    tile = 32

    def norm(src, at, to):
        wide_x = src[pl.ds(at, tile), :].astype(F32)
        scale = lax.rsqrt(jnp.mean(wide_x * wide_x, -1, keepdims=True) + 1e-6)
        a_s[pl.ds(to, tile), :] = (wide_x * scale * gain).astype(BF16)

    ring(0, True)
    lax.fori_loop(0, own // tile, lambda i, _: norm(xr_s, _at(i, tile), pl.multiple_of(k * own + i * tile, tile)), None)
    ring(1, False)
    pltpu.make_async_copy(a_s.at[other, :], a_s.at[other, :], x_sem.at[2]).wait()

    def norm_other(i, _):
        at = pl.multiple_of((1 - k) * own + i * tile, tile)
        norm(a_s, at, at)

    lax.fori_loop(0, own // tile, norm_other, None)
    ring(2, False)
    for i in range(KVH):
        top_s[i : i + 1, :] = jnp.full((1, GROUP * tokens), NEG, F32)
        mix_s[i] = jnp.zeros((HEAD + 8, GROUP * tokens), F32)

    def project(w_ref, col, turn, put):
        def some(t, _):
            at = pl.ds(_at(t, 512), 512)
            out = jnp.dot(a_s[at, :], w_ref[:, col : col + HEAD], preferred_element_type=F32).astype(BF16)
            if turn:
                cos, sin = cos_ref[at, :], sin_ref[at, :]
                lo, up_ = out[:, : HEAD // 2].astype(F32), out[:, HEAD // 2 :].astype(F32)
                out = jnp.concatenate([lo * cos - up_ * sin, up_ * cos + lo * sin], -1).astype(BF16)
            put(at, t, out)

        lax.fori_loop(0, tokens // 512, some, None)

    def pass_on(o, way, p, step):
        remote(kv_s.at[o, way, p], kv_s.at[o, way, p], ks_sem.at[way, p], kr_sem.at[way, p, step], (right, left)[way]).start()

    arrived(0)
    across_all(1)
    started = None
    for p in range(2):
        for i in range(KVH):
            def put(at, t, out):
                kv_s[c, i, p, at, :] = out

            project(wa_s, p * KVH * HEAD + i * HEAD, p == 0, put)
            if started is not None and n > 1:
                pass_on(c, *started, 0)
            started = (i, p)
    if n > 1:
        pass_on(c, *started, 0)

    def queries():
        for h in range(KVH * GROUP):
            def put(at, t, out):
                q_s[h // GROUP, pl.ds(pl.multiple_of((h % GROUP) * tokens + t * 512, 512), 512), :] = out

            project(wqf_s, h * HEAD, True, put)

    e = HEAD**-0.5 * LOG2E
    ones = jnp.ones((8, BK), BF16)

    def block(i, o, key, strips, masked):
        kk = kv_s[o, i, 0, pl.ds(key, BK), :]
        scores = [_dot(kk, q_s[i, at : at + STRIP, :], 1, 1) for at in strips]
        weights, keeps = [], []
        for at, s in zip(strips, scores):
            first = at % tokens
            if masked and first < key + BK - 1:
                gap = lax.broadcasted_iota(jnp.int32, (BK, STRIP), 1) - lax.broadcasted_iota(jnp.int32, (BK, STRIP), 0)
                s = jnp.where(gap >= key - first, s, HIDDEN)
            old = top_s[i : i + 1, at : at + STRIP]
            top = jnp.maximum(old, s.max(axis=0, keepdims=True))
            top_s[i : i + 1, at : at + STRIP] = top
            weights.append(jnp.exp2((s - top) * e).astype(BF16))
            keeps.append(jnp.exp2((old - top) * e))
        values = jnp.concatenate([kv_s[o, i, 1, pl.ds(key, BK), :].T, ones], axis=0)
        for at, p, keep in zip(strips, weights, keeps):
            mix_s[i, :, at : at + STRIP] = mix_s[i, :, at : at + STRIP] * keep + _dot(values, p, 1, 0)

    every = list(range(0, GROUP * tokens, STRIP))

    def own_chunk():
        for i in range(KVH):
            for key in range(0, tokens, BK):
                block(i, c, key, [at for at in every if at % tokens + STRIP > key], True)

    def chunk(s):
        for i in range(KVH):
            o = lax.rem(c + n - s, n) if i == 0 else lax.rem(c + s, n)

            @pl.when(c >= s if i == 0 else c + s >= n)
            def _():
                lax.fori_loop(0, tokens // BK, lambda j, _: block(i, o, _at(j, BK), every, False), None)

    def share_wo():
        arrived(2)

        def send(o, _):
            at = pl.ds(pl.multiple_of((2 * o + k) * rows_o, 16), rows_o)
            remote(wof_s.at[at, :], wof_s.at[at, :], wo_sem.at[0], wo_sem.at[1], sib).start()

        lax.fori_loop(0, n, send, None)

    def take(s, p):
        for way in range(2):
            o = lax.rem(c + n - s, n) if way == 0 else lax.rem(c + s, n)
            pltpu.make_async_copy(kv_s.at[o, way, p], kv_s.at[o, way, p], kr_sem.at[way, p, s - 1]).wait()
            if s < n - 1:
                pass_on(o, way, p, s)

    todo = ["q", "own", *range(1, n)]
    shared = False
    for s in range(1, n):
        for p in range(2):
            take(s, p)
            if (s, p) < (min(2, n - 1), 1):
                continue
            if s == min(5, n - 1) and p == 1:
                share_wo()
                shared = True
            elif todo and (isinstance(todo[0], str) or todo[0] < s or (todo[0] == s and p == 1)):
                task = todo.pop(0)
                if task == "q":
                    arrived(1)
                    across_all(2)
                    queries()
                elif task == "own":
                    own_chunk()
                else:
                    chunk(task)
    for task in todo:
        own_chunk() if task == "own" else chunk(task)

    for i in range(KVH):
        for h in range(GROUP):
            for kk in range(2):
                cols = pl.ds(h * tokens + kk * own, own)
                out = (mix_s[i, :HEAD, cols] * (1 / mix_s[i, HEAD : HEAD + 1, cols])).T.astype(BF16)
                to = pl.ds((i * GROUP + h) * HEAD, HEAD)

                @pl.when(kk == k)
                def _():
                    o_s[k, :, to] = out

                @pl.when(kk != k)
                def _():
                    os_s[:, to] = out

    o_out = remote(os_s, o_s.at[k], o_sem.at[0], o_sem.at[1], sib)
    o_out.start()
    whole = wof_s.at[pl.ds(0, n * rows_o), :]
    pltpu.make_async_copy(whole, whole, wo_sem.at[1]).wait()
    pltpu.make_async_copy(o_s.at[1 - k], o_s.at[1 - k], o_sem.at[1]).wait()

    def finish(j, _):
        at = pl.ds(_at(j, 256), 256)
        hw = o_s.shape[2]
        out = jnp.dot(o_s[0], wof_s[:hw, at], preferred_element_type=F32) + jnp.dot(o_s[1], wof_s[hw:, at], preferred_element_type=F32)
        y_ref[:, at] = (xr_s[:, at].astype(F32) + out).astype(BF16)

    lax.fori_loop(0, d // 256, finish, None)

    o_out.wait_send()
    x_out.wait_send()
    pltpu.make_async_copy(whole, whole, wo_sem.at[0]).wait()
    for mat in range(3):
        pltpu.make_async_copy(bytes_of(mat), bytes_of(mat), xys_sem.at[mat]).wait()
        for _ in range(1):
            some = (wa_s, wqf_s, wof_s)[mat]
            size = (rows, wide) if mat < 2 else (hi, ho)
            sent = some.at[pl.ds(0, (up + down) * size[0]), pl.ds(0, size[1])]
            pltpu.make_async_copy(sent, sent, zs_sem.at[mat]).wait()

    @pl.when(k == r)
    def _():
        for mat in range(2):
            pltpu.make_async_copy(piece(mat, c), piece(mat, c), pre_send.at[mat]).wait()

    for way in range(2):
        for p in range(2):
            sent = kv_s.at[pl.ds(0, n - 1), way, p]
            pltpu.make_async_copy(sent, sent, ks_sem.at[way, p]).wait()


def solution(mesh):
    dp, sp = mesh.shape["dp"], mesh.shape["sp"]

    def step(x, gain, wq, wk, wv, wo):
        own, d = x.shape
        n = sp // 2
        tokens = 2 * own
        half_d = wq.shape[1] // 2
        up, down = n // 2, (n - 1) // 2
        place = lax.div(lax.axis_index("sp"), 2) * tokens + jnp.arange(tokens)
        hh = HEAD // 2
        angle = place.astype(F32)[:, None] * THETA ** (-jnp.arange(hh, dtype=F32) / hh)
        cos, sin = jnp.cos(angle), jnp.sin(angle)
        vm, any_ = pl.BlockSpec(memory_space=pltpu.VMEM), pl.BlockSpec(memory_space=pl.ANY)
        dma = pltpu.SemaphoreType.DMA
        return pl.pallas_call(
            functools.partial(kernel, dp, sp),
            out_shape=jax.ShapeDtypeStruct((own, d), BF16),
            in_specs=[any_, vm, vm, vm, any_, any_, any_, any_],
            out_specs=vm,
            scratch_shapes=[
                pltpu.VMEM((tokens, d), BF16),
                pltpu.VMEM((own, d), BF16),
                pltpu.VMEM((d, half_d), BF16),
                pltpu.VMEM((d, half_d), BF16),
                pltpu.VMEM((2 * half_d, d), BF16),
                pltpu.VMEM((n, KVH, 2, tokens, HEAD), BF16),
                pltpu.VMEM((KVH, GROUP * tokens, HEAD), BF16),
                pltpu.VMEM((KVH, GROUP * tokens), F32),
                pltpu.VMEM((KVH, HEAD + 8, GROUP * tokens), F32),
                pltpu.VMEM((2, own, half_d), BF16),
                pltpu.VMEM((own, half_d), BF16),
                dma((3,)), dma((3,)), dma((2,)), dma((3, 2, max(up, 1))), dma((3,)), dma((3,)), dma((3,)),
                dma((2, 2, max(n - 1, 1))), dma((2, 2)), dma((2,)), dma((2,)),
            ],
            compiler_params=pltpu.CompilerParams(collective_id=0, has_side_effects=True, vmem_limit_bytes=66 * 10**6),
        )(x, gain[None], cos, sin, wq, wk, wv, wo)

    tokens, whole = P(("dp", "sp"), None), P("sp", None)
    return jax.shard_map(
        step,
        mesh=mesh,
        in_specs=(tokens, P(None), whole, whole, whole, whole),
        out_specs=tokens,
        check_vma=False,
    )
```

```python
import functools
import math

import jax
import jax.numpy as jnp
import numpy as np
from jax import lax
from jax.experimental import pallas as pl
from jax.experimental.pallas import tpu as pltpu
from jax.sharding import PartitionSpec as P

HEAD = 256
THETA = 10000
KVH = 2
GROUP = 2
NEG = -1e30
HIDDEN = 2 * NEG
LOG2E = 1.4426950408889634
BK = 512
STRIP = 512
MESH = pl.DeviceIdType.MESH
F32, BF16 = jnp.float32, jnp.bfloat16


def _dot(a, b, ca, cb):
    return lax.dot_general(a, b, (((ca,), (cb,)), ((), ())), preferred_element_type=F32)


def _at(i, unit):
    return pl.multiple_of(i * unit, unit) if not isinstance(i, int) else i * unit


def kernel(dp, sp, x_ref, gain_ref, freq_ref, wq_ref, wk_ref, wv_ref, wo_ref, y_ref,
           a_s, xr_s, cos_s, sin_s, wa_s, wqf_s, wof_s, kv_s, q_s, top_s, mix_s, o_s, os_s,
           x_sem, pre_sem, pre_send, zr_sem, zs_sem, near_sem, far_sem, xys_sem, kr_sem, ks_sem, o_sem, wo_sem):
    g, me = lax.axis_index("dp"), lax.axis_index("sp")
    n = sp // 2
    m = math.isqrt(dp)
    c, k = lax.div(me, 2), lax.rem(me, 2)
    gx, gy = lax.div(g, m), lax.rem(g, m)
    sib = (g, 2 * c + 1 - k)
    right = (g, 2 * lax.rem(c + 1, n) + k)
    left = (g, 2 * lax.rem(c + n - 1, n) + k)
    own, d = x_ref.shape
    rows, rows_o = wq_ref.shape[0], wo_ref.shape[0]
    tokens = 2 * own
    half = wa_s.shape[1]
    up, down = n // 2, (n - 1) // 2

    def remote(src, dst, ssem, rsem, dev):
        return pltpu.make_async_remote_copy(src_ref=src, dst_ref=dst, send_sem=ssem, recv_sem=rsem, device_id=dev, device_id_type=MESH)

    def await_(ref, sem):
        pltpu.make_async_copy(ref, ref, sem).wait()

    def row(p):
        return gx * m + lax.rem(gy + p, m)

    def column(p):
        return lax.rem(gx + p, m) * m + gy

    barrier = pltpu.get_barrier_semaphore()
    for dev in (sib, left, right):
        pl.semaphore_signal(barrier, inc=1, device_id=dev, device_id_type=MESH)
    for p in range(1, m):
        for other_g in (row(p), column(p)):
            pl.semaphore_signal(barrier, inc=1, device_id=(other_g, me), device_id_type=MESH)
    pl.semaphore_wait(barrier, 3 + 2 * (m - 1))

    wide = 2 * half // dp
    sub = min(wide, half // 2)
    hi, ho = rows_o // (dp // 2), d // 2

    def share(v):
        return lax.div(v, dp // 2), lax.rem(v, dp // 2)

    def piece(mat, o, v):
        r, b = share(v)
        if mat < 2:
            return (wa_s, wqf_s)[mat].at[pl.ds(pl.multiple_of((2 * o + r) * rows, 16), rows), pl.ds(pl.multiple_of(b * wide, 128), wide)]
        return wof_s.at[pl.ds(pl.multiple_of((2 * o + k) * rows_o + b * hi, 16), hi), pl.ds(pl.multiple_of(r * ho, 128), ho)]

    def several(mat, count):
        if mat < 2:
            full = dp * n
            h, w = n * 2 * rows, half
        else:
            full = dp * n
            h, w = n * rows_o, d
        ref = (wa_s, wqf_s, wof_s)[mat]
        if h * count % full == 0 and h * count // full % 16 == 0:
            return ref.at[pl.ds(0, h * count // full), :]
        tall, broad = (rows, wide) if mat < 2 else (hi, ho)
        return ref.at[pl.ds(0, tall * count), pl.ds(0, broad)]

    r, b = share(g)

    def sources(mat, kk, i):
        at = b * wide + i * sub
        if mat == 1:
            return [(None, wq_ref.at[:, pl.ds(pl.multiple_of(kk * half + at, 128), sub)])]
        h2 = half // 2
        return [(at < h2, wk_ref.at[:, pl.ds(pl.multiple_of(kk * h2 + lax.rem(at, h2), 128), sub)]),
                (at >= h2, wv_ref.at[:, pl.ds(pl.multiple_of(kk * h2 + lax.rem(at, h2), 128), sub)])]

    def maybe(cond, f):
        f() if cond is None else pl.when(cond)(f)

    def begin(mat):
        if mat == 2:
            src = wo_ref.at[pl.ds(pl.multiple_of(b * hi, 16), hi), pl.ds(pl.multiple_of(r * ho, 128), ho)]
            pltpu.make_async_copy(src, piece(2, c, g), pre_sem.at[2]).start()
            return

        @pl.when(k == r)
        def _():
            for i in range(wide // sub):
                for cond, src in sources(mat, 1 - k, i):
                    maybe(cond, lambda: remote(src, piece(mat, c, g).at[:, pl.ds(i * sub, sub)], pre_send.at[mat], pre_sem.at[mat], sib).start())
                for cond, src in sources(mat, k, i):
                    maybe(cond, lambda: pltpu.make_async_copy(src, piece(mat, c, g).at[:, pl.ds(i * sub, sub)], pre_sem.at[mat]).start())

    def hop(mat, o, way, step):
        remote(piece(mat, o, g), piece(mat, o, g), zs_sem.at[mat], zr_sem.at[mat, way, step], (right, left)[way]).start()

    def across(mat, o):
        first = lax.rem(o, 2)
        for p in range(1, m):
            near, far = jnp.where(first == 0, row(p), column(p)), jnp.where(first == 0, column(p), row(p))
            remote(piece(mat, o, g), piece(mat, o, g), xys_sem.at[mat], near_sem.at[mat, o], (near, me)).start()
            remote(piece(mat, o, g), piece(mat, o, g), xys_sem.at[mat], far_sem.at[mat], (far, me)).start()

    def hand_on(mat, o):
        first = lax.rem(o, 2)
        await_(several(mat, m - 1), near_sem.at[mat, o])
        for q in range(1, m):
            for p in range(1, m):
                v, far = jnp.where(first == 0, row(q), column(q)), jnp.where(first == 0, column(p), row(p))
                remote(piece(mat, o, v), piece(mat, o, v), xys_sem.at[mat], far_sem.at[mat], (far, me)).start()

    def for_chips(f, mat):
        lax.fori_loop(0, n, lambda o, _: f(mat, o), None)

    def arrived(mat):
        await_(several(mat, n * m * (m - 1)), far_sem.at[mat])

    def ring(mat, s, f=None):
        for way, last in ((0, up), (1, down)):
            if s <= last:
                o = lax.rem(c + n - s, n) if way == 0 else lax.rem(c + s, n)
                await_(piece(mat, o, g), zr_sem.at[mat, way, s - 1])
                if s < last:
                    hop(mat, o, way, s)
                if f is not None:
                    f(mat, o)

    def set_out(mat):
        await_(piece(mat, c, g), pre_sem.at[mat])
        if up:
            hop(mat, c, 0, 0)
        if down:
            hop(mat, c, 1, 0)

    mine = pl.ds(pl.multiple_of(k * own, own), own)
    other = pl.ds(pl.multiple_of((1 - k) * own, own), own)
    begin(0)
    begin(1)
    begin(2)
    x_in = pltpu.make_async_copy(x_ref, xr_s, x_sem.at[0])
    x_in.start()
    x_out = remote(x_ref, a_s.at[mine, :], x_sem.at[1], x_sem.at[2], sib)
    x_out.start()
    set_out(0)
    across(0, c)
    set_out(1)
    set_out(2)
    x_in.wait()

    gain = gain_ref[...].astype(F32).reshape(1, d)
    tile = 32

    def norm(src, at, to):
        wide_x = src[pl.ds(at, tile), :].astype(F32)
        scale = lax.rsqrt(jnp.mean(wide_x * wide_x, -1, keepdims=True) + 1e-6)
        a_s[pl.ds(to, tile), :] = (wide_x * scale * gain).astype(BF16)

    def norm_own(i, _):
        norm(xr_s, _at(i, tile), pl.multiple_of(k * own + i * tile, tile))

    def norm_other(i, _):
        at = pl.multiple_of((1 - k) * own + i * tile, tile)
        norm(a_s, at, at)

    def angles(i, _):
        at = pl.ds(_at(i, 64), 64)
        place = c * tokens + i * 64 + lax.broadcasted_iota(jnp.int32, (64, HEAD // 2), 0)
        angle = place.astype(F32) * freq_ref[...]
        cos_s[at, :] = jnp.cos(angle)
        sin_s[at, :] = jnp.sin(angle)

    steps = own // tile
    lax.fori_loop(0, steps, norm_own, None)
    for s in range(1, up + 1):
        ring(0, s, across)
        if s == 1:
            hand_on(0, c)
            await_(a_s.at[other, :], x_sem.at[2])
            lax.fori_loop(0, steps, norm_other, None)
        else:
            ring(1, s - 1)
            ring(2, s - 1)
            for way, last in ((0, up), (1, down)):
                if s - 1 <= last:
                    hand_on(0, lax.rem(c + n - s + 1, n) if way == 0 else lax.rem(c + s - 1, n))
            lax.fori_loop((s - 2) * tokens // 64 // max(up - 1, 1), (s - 1) * tokens // 64 // max(up - 1, 1), angles, None)
    if up == 1:
        lax.fori_loop(0, tokens // 64, angles, None)
    for i in range(KVH):
        top_s[i] = jnp.full((1, GROUP * tokens), NEG, F32)
        mix_s[i] = jnp.zeros((HEAD + 8, GROUP * tokens), F32)
    for way, last in ((0, up), (1, down)):
        if up <= last:
            hand_on(0, lax.rem(c + n - up, n) if way == 0 else lax.rem(c + up, n))
    ring(1, up)
    ring(2, up)

    def project(w_ref, col, t, turn):
        at = pl.ds(_at(t, BK), BK)
        out = jnp.dot(a_s[at, :], w_ref[:, pl.ds(pl.multiple_of(col, HEAD), HEAD)], preferred_element_type=F32).astype(BF16)
        if turn:
            cos, sin = cos_s[at, :], sin_s[at, :]
            lo, up_ = out[:, : HEAD // 2].astype(F32), out[:, HEAD // 2 :].astype(F32)
            out = jnp.concatenate([lo * cos - up_ * sin, up_ * cos + lo * sin], -1).astype(BF16)
        return out

    def pass_on(o, way, p, step):
        remote(kv_s.at[o, way, p], kv_s.at[o, way, p], ks_sem.at[way], kr_sem.at[way, p, step], (right, left)[way]).start()

    parts = tokens // BK
    pieces = 2 * parts

    arrived(0)
    for_chips(across, 1)

    def own_keys(t, _):
        for p in range(2):
            def one(i, _):
                kv_s[c, i, 2 * t + p] = project(wa_s, (p * KVH + i) * HEAD, t, p == 0)

            lax.fori_loop(0, KVH, one, None)
            for i in range(KVH):
                pass_on(c, i, 2 * t + p, 0)

    lax.fori_loop(0, parts, own_keys, None)

    def queries():
        def one(h, _):
            def some(t, _):
                at = pl.ds(pl.multiple_of(lax.rem(h, GROUP) * tokens + t * BK, BK), BK)
                q_s[lax.div(h, GROUP), at, :] = project(wqf_s, h * HEAD, t, True)

            lax.fori_loop(0, tokens // BK, some, None)

        lax.fori_loop(0, KVH * GROUP, one, None)

    e = HEAD**-0.5 * LOG2E
    ones = jnp.ones((8, BK), BF16)

    def block(i, o, j, strips, masked):
        kk = kv_s[o, i, 2 * j]
        scores = [_dot(kk, q_s[i, at : at + STRIP, :], 1, 1) for at in strips]
        weights, keeps = [], []
        for at, s in zip(strips, scores):
            if masked and at % tokens < (j + 1) * BK - 1:
                gap = lax.broadcasted_iota(jnp.int32, (BK, STRIP), 1) - lax.broadcasted_iota(jnp.int32, (BK, STRIP), 0)
                s = jnp.where(gap >= j * BK - at % tokens, s, HIDDEN)
            old = top_s[i, :, at : at + STRIP]
            top = jnp.maximum(old, s.max(axis=0, keepdims=True))
            top_s[i, :, at : at + STRIP] = top
            weights.append(jnp.exp2((s - top) * e).astype(BF16))
            keeps.append(jnp.exp2((old - top) * e))
        values = jnp.concatenate([kv_s[o, i, 2 * j + 1].T, ones], axis=0)
        for at, p, keep in zip(strips, weights, keeps):
            mix_s[i, :, at : at + STRIP] = mix_s[i, :, at : at + STRIP] * keep + _dot(values, p, 1, 0)

    every = list(range(0, GROUP * tokens, STRIP))

    def own_chunk():
        def one(i, _):
            for j in range(parts):
                block(i, c, j, [at for at in every if at % tokens + STRIP > j * BK], True)

        lax.fori_loop(0, KVH, one, None)

    def origin(way, s):
        return lax.rem(jnp.where(way == 0, c + n - s, c + s), n)

    def unit(u, _):
        s, j = lax.div(u, parts) + 1, lax.rem(u, parts)

        def one(i, _):
            @pl.when(origin(i, s) < c)
            def _():
                block(i, origin(i, s), j, every, False)

        lax.fori_loop(0, KVH, one, None)

    def share_wo():
        arrived(2)

        def send(o, _):
            at = pl.ds(pl.multiple_of((2 * o + k) * rows_o, 16), rows_o)
            remote(wof_s.at[at, :], wof_s.at[at, :], wo_sem.at[0], wo_sem.at[1], sib).start()

        lax.fori_loop(0, n, send, None)

    def take(q):
        s, p = lax.div(q, pieces) + 1, lax.rem(q, pieces)
        for way in range(2):
            o = origin(way, s)
            await_(kv_s.at[o, way, p], kr_sem.at[way, p, s - 1])

            @pl.when(s < n - 1)
            def _():
                pass_on(o, way, p, s)

    end = pieces * (n - 1)
    at_wq, at_q, at_own, at_wo, at_share = (min(i, end - 1) for i in (2, 5, 6, 9, 14))

    def main(q, done):
        take(q)

        @pl.when(q == at_wq)
        def _():
            for_chips(hand_on, 1)

        @pl.when(q == at_q)
        def _():
            arrived(1)
            for_chips(across, 2)
            queries()

        @pl.when(q == at_own)
        def _():
            own_chunk()

        @pl.when(q == at_wo)
        def _():
            for_chips(hand_on, 2)

        @pl.when(q == at_share)
        def _():
            share_wo()

        until = jnp.where(q > at_own, jnp.minimum(done + 2, lax.div(q + 1, 2)), 0)
        lax.fori_loop(done, until, unit, None)
        return until

    done = lax.fori_loop(0, end, main, jnp.int32(0))
    lax.fori_loop(done, end // 2, unit, None)

    def result(j, at):
        i, h = lax.div(j, GROUP), lax.rem(j, GROUP)
        cols = pl.ds(pl.multiple_of(h * tokens + at, own), own)
        return (mix_s[i, :HEAD, cols] * (1 / mix_s[i, HEAD : HEAD + 1, cols])).T.astype(BF16)

    def theirs(j, _):
        os_s[j] = result(j, (1 - k) * own)

    def ours(j, _):
        o_s[k, j] = result(j, k * own)

    heads = KVH * GROUP
    lax.fori_loop(0, heads, theirs, None)
    o_out = remote(os_s, o_s.at[k], o_sem.at[0], o_sem.at[1], sib)
    o_out.start()
    lax.fori_loop(0, heads, ours, None)
    whole = wof_s.at[pl.ds(0, n * rows_o), :]
    await_(whole, wo_sem.at[1])
    await_(o_s.at[1 - k], o_sem.at[1])

    def finish(j, _):
        at = pl.ds(_at(j, 256), 256)
        out = xr_s[:, at].astype(F32)
        seen = jnp.concatenate([o_s[kk, h] for kk in range(2) for h in range(heads)], axis=1)
        y_ref[:, at] = (out + jnp.dot(seen, wof_s[:, at], preferred_element_type=F32)).astype(BF16)

    lax.fori_loop(0, d // 256, finish, None)

    o_out.wait_send()
    x_out.wait_send()
    await_(whole, wo_sem.at[0])
    for mat in range(3):
        await_(several(mat, n * (dp - 1)), xys_sem.at[mat])
        if up:
            await_(several(mat, up + down), zs_sem.at[mat])

    @pl.when(k == r)
    def _():
        for mat in range(2):
            await_(piece(mat, c, g), pre_send.at[mat])

    for way in range(2):
        await_(kv_s.at[pl.ds(0, n - 1), way], ks_sem.at[way])


def solution(mesh):
    dp, sp = mesh.shape["dp"], mesh.shape["sp"]

    def step(x, gain, wq, wk, wv, wo):
        own, d = x.shape
        n = sp // 2
        tokens = 2 * own
        half_d = wq.shape[1] // 2
        up, down = n // 2, (n - 1) // 2
        hh = HEAD // 2
        freq = (THETA ** (-np.arange(hh, dtype=np.float32) / hh)).astype(np.float32)[None]
        vm, any_ = pl.BlockSpec(memory_space=pltpu.VMEM), pl.BlockSpec(memory_space=pl.ANY)
        dma = pltpu.SemaphoreType.DMA
        return pl.pallas_call(
            functools.partial(kernel, dp, sp),
            out_shape=jax.ShapeDtypeStruct((own, d), BF16),
            in_specs=[any_, vm, vm, any_, any_, any_, any_],
            out_specs=vm,
            scratch_shapes=[
                pltpu.VMEM((tokens, d), BF16),
                pltpu.VMEM((own, d), BF16),
                pltpu.VMEM((tokens, hh), F32),
                pltpu.VMEM((tokens, hh), F32),
                pltpu.VMEM((d, half_d), BF16),
                pltpu.VMEM((d, half_d), BF16),
                pltpu.VMEM((2 * half_d, d), BF16),
                pltpu.VMEM((n, KVH, 2 * tokens // BK, BK, HEAD), BF16),
                pltpu.VMEM((KVH, GROUP * tokens, HEAD), BF16),
                pltpu.VMEM((KVH, 1, GROUP * tokens), F32),
                pltpu.VMEM((KVH, HEAD + 8, GROUP * tokens), F32),
                pltpu.VMEM((2, KVH * GROUP, own, HEAD), BF16),
                pltpu.VMEM((KVH * GROUP, own, HEAD), BF16),
                dma((3,)), dma((3,)), dma((2,)), dma((3, 2, max(up, 1))), dma((3,)), dma((3, n)), dma((3,)), dma((3,)),
                dma((2, 2 * tokens // BK, max(n - 1, 1))), dma((2,)), dma((2,)), dma((2,)),
            ],
            compiler_params=pltpu.CompilerParams(collective_id=0, has_side_effects=True, vmem_limit_bytes=66 * 10**6),
        )(x, gain, freq, wq, wk, wv, wo)

    tokens, whole = P(("dp", "sp"), None), P("sp", None)
    return jax.shard_map(
        step,
        mesh=mesh,
        in_specs=(tokens, P(None), whole, whole, whole, whole),
        out_specs=tokens,
        check_vma=False,
    )
```

```python
import functools
import math

import jax
import jax.numpy as jnp
import numpy as np
from jax import lax
from jax.experimental import pallas as pl
from jax.experimental.pallas import tpu as pltpu
from jax.sharding import PartitionSpec as P

HEAD = 256
THETA = 10000
KVH = 2
GROUP = 2
NEG = -1e30
HIDDEN = 2 * NEG
LOG2E = 1.4426950408889634
BK = 512
STRIP = 512
MESH = pl.DeviceIdType.MESH
F32, BF16 = jnp.float32, jnp.bfloat16


def _dot(a, b, ca, cb):
    return lax.dot_general(a, b, (((ca,), (cb,)), ((), ())), preferred_element_type=F32)


def _at(i, unit):
    return pl.multiple_of(i * unit, unit) if not isinstance(i, int) else i * unit


def kernel(dp, sp, x_ref, gain_ref, freq_ref, wq_ref, wk_ref, wv_ref, wo_ref, y_ref,
           a_s, xr_s, cos_s, sin_s, wa_s, wqf_s, wof_s, kv_s, q_s, top_s, mix_s, o_s, os_s,
           x_sem, pre_sem, pre_send, zr_sem, zs_sem, near_sem, far_sem, xys_sem, kr_sem, ks_sem, o_sem, wo_sem):
    g, me = lax.axis_index("dp"), lax.axis_index("sp")
    n = sp // 2
    m = math.isqrt(dp)
    c, k = lax.div(me, 2), lax.rem(me, 2)
    gx, gy = lax.div(g, m), lax.rem(g, m)
    sib = (g, 2 * c + 1 - k)
    right = (g, 2 * lax.rem(c + 1, n) + k)
    left = (g, 2 * lax.rem(c + n - 1, n) + k)
    own, d = x_ref.shape
    rows, rows_o = wq_ref.shape[0], wo_ref.shape[0]
    tokens = 2 * own
    half = wa_s.shape[1]
    up, down = n // 2, (n - 1) // 2

    def remote(src, dst, ssem, rsem, dev):
        return pltpu.make_async_remote_copy(src_ref=src, dst_ref=dst, send_sem=ssem, recv_sem=rsem, device_id=dev, device_id_type=MESH)

    def await_(ref, sem):
        pltpu.make_async_copy(ref, ref, sem).wait()

    def row(p):
        return gx * m + lax.rem(gy + p, m)

    def column(p):
        return lax.rem(gx + p, m) * m + gy

    barrier = pltpu.get_barrier_semaphore()
    for dev in (sib, left, right):
        pl.semaphore_signal(barrier, inc=1, device_id=dev, device_id_type=MESH)
    for p in range(1, m):
        for other_g in (row(p), column(p)):
            pl.semaphore_signal(barrier, inc=1, device_id=(other_g, me), device_id_type=MESH)

    hi, ho = rows_o // (dp // 2), d // 2
    h2 = half // 2
    mats = [(wa_s, 0, half, [wk_ref, wv_ref]), (wqf_s, 0, half, [wq_ref])]
    mq, mo = 1, 2

    def share(v):
        return lax.div(v, dp // 2), lax.rem(v, dp // 2)

    def wide(mat):
        return 2 * mats[mat][2] // dp

    def piece(mat, o, v):
        r, b = share(v)
        if mat < mo:
            ref, col, _, _ = mats[mat]
            return ref.at[pl.ds(pl.multiple_of((2 * o + r) * rows, 16), rows), pl.ds(pl.multiple_of(col + b * wide(mat), 128), wide(mat))]
        return wof_s.at[pl.ds(pl.multiple_of((2 * o + k) * rows_o + b * hi, 16), hi), pl.ds(pl.multiple_of(r * ho, 128), ho)]

    def several(mat, count):
        ref, h, w = (mats[mat][0], n * 2 * rows, mats[mat][2]) if mat < mo else (wof_s, n * rows_o, d)
        if h * count % (dp * n) == 0 and h * count // (dp * n) % 16 == 0:
            return ref.at[pl.ds(0, h * count // (dp * n)), pl.ds(0, w)]
        tall, broad = (rows, wide(mat)) if mat < mo else (hi, ho)
        return ref.at[pl.ds(0, tall * count), pl.ds(0, broad)]

    r, b = share(g)

    def sources(mat, kk):
        _, _, cols, refs = mats[mat]
        each = cols // len(refs)
        at = b * wide(mat)
        for i, ref in enumerate(refs):
            cond = None if len(refs) == 1 else lax.div(at, each) == i
            yield cond, ref.at[:, pl.ds(pl.multiple_of(kk * each + lax.rem(at, each), 128), wide(mat))]

    def maybe(cond, f):
        f() if cond is None else pl.when(cond)(f)

    def begin_here(mat):
        if mat == mo:
            src = wo_ref.at[pl.ds(pl.multiple_of(b * hi, 16), hi), pl.ds(pl.multiple_of(r * ho, 128), ho)]
            pltpu.make_async_copy(src, piece(mo, c, g), pre_sem.at[mo]).start()
            return

        @pl.when(k == r)
        def _():
            for cond, src in sources(mat, k):
                maybe(cond, lambda: pltpu.make_async_copy(src, piece(mat, c, g), pre_sem.at[mat]).start())

    def begin_there(mat):
        @pl.when(k == r)
        def _():
            for cond, src in sources(mat, 1 - k):
                maybe(cond, lambda: remote(src, piece(mat, c, g), pre_send.at[mat], pre_sem.at[mat], sib).start())

    def hop(mat, o, way, step):
        remote(piece(mat, o, g), piece(mat, o, g), zs_sem.at[mat], zr_sem.at[mat, way, step], (right, left)[way]).start()

    def across(mat, o):
        first = lax.rem(o, 2)
        for p in range(1, m):
            near, far = jnp.where(first == 0, row(p), column(p)), jnp.where(first == 0, column(p), row(p))
            remote(piece(mat, o, g), piece(mat, o, g), xys_sem.at[mat], near_sem.at[mat, o], (near, me)).start()
            remote(piece(mat, o, g), piece(mat, o, g), xys_sem.at[mat], far_sem.at[mat], (far, me)).start()

    def hand_on(mat, o):
        first = lax.rem(o, 2)
        await_(several(mat, m - 1), near_sem.at[mat, o])
        for q in range(1, m):
            for p in range(1, m):
                v, far = jnp.where(first == 0, row(q), column(q)), jnp.where(first == 0, column(p), row(p))
                remote(piece(mat, o, v), piece(mat, o, v), xys_sem.at[mat], far_sem.at[mat], (far, me)).start()

    def for_chips(f, mat):
        lax.fori_loop(0, n, lambda o, _: f(mat, o), None)

    def arrived(mat):
        await_(several(mat, n * m * (m - 1)), far_sem.at[mat])

    def ring(mat, s, f=None):
        for way, last in ((0, up), (1, down)):
            if s <= last:
                o = lax.rem(c + n - s, n) if way == 0 else lax.rem(c + s, n)
                await_(piece(mat, o, g), zr_sem.at[mat, way, s - 1])
                if s < last:
                    hop(mat, o, way, s)
                if f is not None:
                    f(mat, o)

    def set_out(mat):
        await_(piece(mat, c, g), pre_sem.at[mat])
        if up:
            hop(mat, c, 0, 0)
        if down:
            hop(mat, c, 1, 0)

    gain = gain_ref[...].astype(F32).reshape(1, d)
    tile = 32

    def norm(src, at, to):
        wide_x = src[pl.ds(at, tile), :].astype(F32)
        scale = lax.rsqrt(jnp.mean(wide_x * wide_x, -1, keepdims=True) + 1e-6)
        a_s[pl.ds(to, tile), :] = (wide_x * scale * gain).astype(BF16)

    def norm_own(i, _):
        norm(xr_s, _at(i, tile), pl.multiple_of(k * own + i * tile, tile))

    def norm_other(i, _):
        at = pl.multiple_of((1 - k) * own + i * tile, tile)
        norm(a_s, at, at)

    def angles(i, _):
        at = pl.ds(_at(i, 64), 64)
        place = c * tokens + i * 64 + lax.broadcasted_iota(jnp.int32, (64, HEAD // 2), 0)
        angle = place.astype(F32) * freq_ref[...]
        cos_s[at, :] = jnp.cos(angle)
        sin_s[at, :] = jnp.sin(angle)

    steps = own // tile
    for mat in range(3):
        begin_here(mat)
    x_in = pltpu.make_async_copy(x_ref, xr_s, x_sem.at[0])
    x_in.start()
    pl.semaphore_wait(barrier, 3 + 2 * (m - 1))
    begin_there(0)
    begin_there(1)
    x_out = remote(x_ref, a_s.at[pl.ds(pl.multiple_of(k * own, own), own), :], x_sem.at[1], x_sem.at[2], sib)
    x_out.start()
    set_out(0)
    across(0, c)
    set_out(1)
    x_in.wait()
    lax.fori_loop(0, steps, norm_own, None)

    def both(step):
        if step == 0:
            return [c]
        return [lax.rem(c + n - step, n)] * (step <= up) + [lax.rem(c + step, n)] * (step <= down)

    def hand_on_all(step):
        for o in both(step):
            hand_on(0, o)

    tiles, spread = tokens // 64, max(up - 1, 1)
    for s in range(1, up + 1):
        ring(0, s, across)
        if s == 1:
            set_out(mo)
        elif s == 2:
            ring(mq, 1)
        elif s == 3:
            ring(mo, 1)
        else:
            ring(mq, s - 2)
            ring(mo, s - 2)
        hand_on_all(s - 1)
        if s == 1:
            await_(a_s.at[pl.ds(pl.multiple_of((1 - k) * own, own), own), :], x_sem.at[2])
            lax.fori_loop(0, steps, norm_other, None)
        if s > 1 or up == 1:
            lax.fori_loop((s - 2) * tiles // spread if up > 1 else 0, (s - 1) * tiles // spread if up > 1 else tiles, angles, None)
    rest = [(mat, s) for s in range(1, up + 1) for mat in (mq, mo) if not (s <= up - 2 or (s == 1 and up >= (2 if mat == mq else 3)))]
    handed = False
    for mat, s in rest[:-1]:
        ring(mat, s)
        if not handed:
            hand_on_all(up)
            handed = True
    if not handed:
        hand_on_all(up)
    for i in range(KVH):
        top_s[i] = jnp.full((1, GROUP * tokens), NEG, F32)
        mix_s[i] = jnp.zeros((HEAD + 8, GROUP * tokens), F32)

    def project(w_ref, col, t, turn):
        at = pl.ds(_at(t, BK), BK)
        out = jnp.dot(a_s[at, :], w_ref[:, pl.ds(pl.multiple_of(col, HEAD), HEAD)], preferred_element_type=F32).astype(BF16)
        if turn:
            cos, sin = cos_s[at, :], sin_s[at, :]
            lo, up_ = out[:, : HEAD // 2].astype(F32), out[:, HEAD // 2 :].astype(F32)
            out = jnp.concatenate([lo * cos - up_ * sin, up_ * cos + lo * sin], -1).astype(BF16)
        return out

    def pass_on(o, way, p, step):
        remote(kv_s.at[o, way, p], kv_s.at[o, way, p], ks_sem.at[way], kr_sem.at[way, p, step], (right, left)[way]).start()

    parts = tokens // BK
    pieces = 2 * parts

    def own_keys(t, _):
        for p in range(2):
            def one(i, _):
                kv_s[c, i, 2 * t + p] = project(wa_s, (p * KVH + i) * HEAD, t, p == 0)

            lax.fori_loop(0, KVH, one, None)
            for i in range(KVH):
                pass_on(c, i, 2 * t + p, 0)

    arrived(0)
    for_chips(across, mq)
    lax.fori_loop(0, parts, own_keys, None)
    for mat, s in rest[-1:]:
        ring(mat, s)

    def queries():
        def one(h, _):
            def some(t, _):
                at = pl.ds(pl.multiple_of(lax.rem(h, GROUP) * tokens + t * BK, BK), BK)
                q_s[lax.div(h, GROUP), at, :] = project(wqf_s, h * HEAD, t, True)

            lax.fori_loop(0, tokens // BK, some, None)

        lax.fori_loop(0, KVH * GROUP, one, None)

    e = HEAD**-0.5 * LOG2E
    ones = jnp.ones((8, BK), BF16)

    def block(i, o, j, strips, masked):
        kk = kv_s[o, i, 2 * j]
        scores = [_dot(kk, q_s[i, at : at + STRIP, :], 1, 1) for at in strips]
        weights, keeps = [], []
        for at, s in zip(strips, scores):
            if masked and at % tokens < (j + 1) * BK - 1:
                gap = lax.broadcasted_iota(jnp.int32, (BK, STRIP), 1) - lax.broadcasted_iota(jnp.int32, (BK, STRIP), 0)
                s = jnp.where(gap >= j * BK - at % tokens, s, HIDDEN)
            old = top_s[i, :, at : at + STRIP]
            top = jnp.maximum(old, s.max(axis=0, keepdims=True))
            top_s[i, :, at : at + STRIP] = top
            weights.append(jnp.exp2((s - top) * e).astype(BF16))
            keeps.append(jnp.exp2((old - top) * e))
        values = jnp.concatenate([kv_s[o, i, 2 * j + 1].T, ones], axis=0)
        for at, p, keep in zip(strips, weights, keeps):
            mix_s[i, :, at : at + STRIP] = mix_s[i, :, at : at + STRIP] * keep + _dot(values, p, 1, 0)

    every = list(range(0, GROUP * tokens, STRIP))

    def own_chunk():
        def one(i, _):
            for j in range(parts):
                block(i, c, j, [at for at in every if at % tokens + STRIP > j * BK], True)

        lax.fori_loop(0, KVH, one, None)

    def origin(way, s):
        return lax.rem(jnp.where(way == 0, c + n - s, c + s), n)

    def unit(u, _):
        s, j = lax.div(u, parts) + 1, lax.rem(u, parts)

        def one(i, _):
            @pl.when(origin(i, s) < c)
            def _():
                block(i, origin(i, s), j, every, False)

        lax.fori_loop(0, KVH, one, None)

    def share_wo():
        arrived(mo)

        def send(o, _):
            at = pl.ds(pl.multiple_of((2 * o + k) * rows_o, 16), rows_o)
            remote(wof_s.at[at, :], wof_s.at[at, :], wo_sem.at[0], wo_sem.at[1], sib).start()

        lax.fori_loop(0, n, send, None)

    def take(q):
        s, p = lax.div(q, pieces) + 1, lax.rem(q, pieces)
        for way in range(2):
            o = origin(way, s)
            await_(kv_s.at[o, way, p], kr_sem.at[way, p, s - 1])

            @pl.when(s < n - 1)
            def _():
                pass_on(o, way, p, s)

    end = pieces * (n - 1)
    at_wq, at_q, at_own, at_wo, at_share = (min(i, end - 1) for i in (2, 5, 6, 9, 14))

    def main(q, done):
        take(q)

        @pl.when(q == at_wq)
        def _():
            for_chips(hand_on, mq)

        @pl.when(q == at_q)
        def _():
            arrived(mq)
            for_chips(across, mo)
            queries()

        @pl.when(q == at_own)
        def _():
            own_chunk()

        @pl.when(q == at_wo)
        def _():
            for_chips(hand_on, mo)

        @pl.when(q == at_share)
        def _():
            share_wo()

        until = jnp.where(q > at_own, jnp.minimum(done + 2, lax.div(q + 1, 2)), 0)
        lax.fori_loop(done, until, unit, None)
        return until

    done = lax.fori_loop(0, end, main, jnp.int32(0))
    lax.fori_loop(done, parts * (n - 1), unit, None)

    def result(j, at):
        i, h = lax.div(j, GROUP), lax.rem(j, GROUP)
        cols = pl.ds(pl.multiple_of(h * tokens + at, own), own)
        return (mix_s[i, :HEAD, cols] * (1 / mix_s[i, HEAD : HEAD + 1, cols])).T.astype(BF16)

    def theirs(j, _):
        os_s[j] = result(j, (1 - k) * own)

    def ours(j, _):
        o_s[k, j] = result(j, k * own)

    heads = KVH * GROUP
    lax.fori_loop(0, heads, theirs, None)
    o_out = remote(os_s, o_s.at[k], o_sem.at[0], o_sem.at[1], sib)
    o_out.start()
    lax.fori_loop(0, heads, ours, None)
    whole = wof_s.at[pl.ds(0, n * rows_o), :]
    await_(whole, wo_sem.at[1])
    hw, col, kept = heads * HEAD, 256, GROUP * tokens // 256

    def product(kk, at):
        seen = jnp.concatenate([o_s[kk, h] for h in range(heads)], axis=1)
        return jnp.dot(seen, wof_s[pl.ds(pl.multiple_of(kk * hw, hw), hw), at], preferred_element_type=F32)

    def half_done(j, _):
        at = pl.ds(_at(j, col), col)
        out = product(k, at)
        for i in range(2):
            mix_s[i, : own // 2, at] = out[i * own // 2 : (i + 1) * own // 2]

    lax.fori_loop(0, min(kept, d // col), half_done, None)
    await_(o_s.at[1 - k], o_sem.at[1])

    def finish(j, _):
        at = pl.ds(_at(j, col), col)
        out = product(1 - k, at)
        for i in range(2):
            part = slice(i * own // 2, (i + 1) * own // 2)
            y_ref[part, at] = (xr_s[part, at].astype(F32) + (mix_s[i, : own // 2, at] + out[part])).astype(BF16)

    lax.fori_loop(0, min(kept, d // col), finish, None)
    for j in range(kept, d // col):
        at = pl.ds(j * col, col)
        y_ref[:, at] = (xr_s[:, at].astype(F32) + (product(k, at) + product(1 - k, at))).astype(BF16)

    o_out.wait_send()
    x_out.wait_send()
    await_(whole, wo_sem.at[0])
    for mat in range(mo + 1):
        await_(several(mat, n * (dp - 1)), xys_sem.at[mat])
        if up:
            await_(several(mat, up + down), zs_sem.at[mat])

    @pl.when(k == r)
    def _():
        for mat in range(mo):
            await_(piece(mat, c, g), pre_send.at[mat])

    for way in range(2):
        await_(kv_s.at[pl.ds(0, n - 1), way], ks_sem.at[way])


def solution(mesh):
    dp, sp = mesh.shape["dp"], mesh.shape["sp"]

    def step(x, gain, wq, wk, wv, wo):
        own, d = x.shape
        n = sp // 2
        tokens = 2 * own
        half_d = wq.shape[1] // 2
        up, down = n // 2, (n - 1) // 2
        hh = HEAD // 2
        freq = (THETA ** (-np.arange(hh, dtype=np.float32) / hh)).astype(np.float32)[None]
        vm, any_ = pl.BlockSpec(memory_space=pltpu.VMEM), pl.BlockSpec(memory_space=pl.ANY)
        dma = pltpu.SemaphoreType.DMA
        return pl.pallas_call(
            functools.partial(kernel, dp, sp),
            out_shape=pltpu.VMEM((own, d), BF16),
            in_specs=[any_, vm, vm, any_, any_, any_, any_],
            out_specs=vm,
            scratch_shapes=[
                pltpu.VMEM((tokens, d), BF16),
                pltpu.VMEM((own, d), BF16),
                pltpu.VMEM((tokens, hh), F32),
                pltpu.VMEM((tokens, hh), F32),
                pltpu.VMEM((d, half_d), BF16),
                pltpu.VMEM((d, half_d), BF16),
                pltpu.VMEM((2 * half_d, d), BF16),
                pltpu.VMEM((n, KVH, 2 * tokens // BK, BK, HEAD), BF16),
                pltpu.VMEM((KVH, GROUP * tokens, HEAD), BF16),
                pltpu.VMEM((KVH, 1, GROUP * tokens), F32),
                pltpu.VMEM((KVH, HEAD + 8, GROUP * tokens), F32),
                pltpu.VMEM((2, KVH * GROUP, own, HEAD), BF16),
                pltpu.VMEM((KVH * GROUP, own, HEAD), BF16),
                dma((3,)), dma((3,)), dma((2,)), dma((3, 2, max(up, 1))), dma((3,)), dma((3, n)), dma((3,)), dma((3,)),
                dma((2, 2 * tokens // BK, max(n - 1, 1))), dma((2,)), dma((2,)), dma((2,)),
            ],
            compiler_params=pltpu.CompilerParams(collective_id=0, has_side_effects=True, vmem_limit_bytes=62 * 10**6),
        )(x, gain, freq, wq, wk, wv, wo)

    tokens, whole = P(("dp", "sp"), None), P("sp", None)
    return jax.shard_map(
        step,
        mesh=mesh,
        in_specs=(tokens, P(None), whole, whole, whole, whole),
        out_specs=tokens,
        check_vma=False,
    )
```

```python
import functools
import math

import jax
import jax.numpy as jnp
import numpy as np
from jax import lax
from jax.experimental import pallas as pl
from jax.experimental.pallas import tpu as pltpu
from jax.sharding import PartitionSpec as P

HEAD = 256
THETA = 10000
KVH = 2
GROUP = 2
NEG = -1e30
HIDDEN = 2 * NEG
LOG2E = 1.4426950408889634
BK = 512
STRIP = 512
MESH = pl.DeviceIdType.MESH
F32, BF16 = jnp.float32, jnp.bfloat16


def _dot(a, b, ca, cb):
    return lax.dot_general(a, b, (((ca,), (cb,)), ((), ())), preferred_element_type=F32)


def _at(i, unit):
    return pl.multiple_of(i * unit, unit) if not isinstance(i, int) else i * unit


def kernel(dp, sp, x_ref, gain_ref, freq_ref, wq_ref, wk_ref, wv_ref, wo_ref, y_ref,
           a_s, xr_s, cos_s, sin_s, wa_s, wqf_s, wof_s, kv_s, q_s, top_s, keep_s, mix_s, o_s, os_s,
           x_sem, pre_sem, pre_send, zr_sem, zs_sem, near_sem, far_sem, xys_sem, kr_sem, ks_sem, o_sem, wo_sem):
    g, me = lax.axis_index("dp"), lax.axis_index("sp")
    n = sp // 2
    m = math.isqrt(dp)
    c, k = lax.div(me, 2), lax.rem(me, 2)
    gx, gy = lax.div(g, m), lax.rem(g, m)
    sib = (g, 2 * c + 1 - k)
    right = (g, 2 * lax.rem(c + 1, n) + k)
    left = (g, 2 * lax.rem(c + n - 1, n) + k)
    own, d = x_ref.shape
    rows, rows_o = wq_ref.shape[0], wo_ref.shape[0]
    tokens = 2 * own
    half = wa_s.shape[1]
    up, down = n // 2, (n - 1) // 2

    def remote(src, dst, ssem, rsem, dev):
        return pltpu.make_async_remote_copy(src_ref=src, dst_ref=dst, send_sem=ssem, recv_sem=rsem, device_id=dev, device_id_type=MESH)

    def await_(ref, sem):
        pltpu.make_async_copy(ref, ref, sem).wait()

    def row(p):
        return gx * m + lax.rem(gy + p, m)

    def column(p):
        return lax.rem(gx + p, m) * m + gy

    barrier = pltpu.get_barrier_semaphore()
    for dev in (sib, left, right):
        pl.semaphore_signal(barrier, inc=1, device_id=dev, device_id_type=MESH)
    for p in range(1, m):
        for other_g in (row(p), column(p)):
            pl.semaphore_signal(barrier, inc=1, device_id=(other_g, me), device_id_type=MESH)

    hi, ho = rows_o // (dp // 2), d // 2
    h2 = half // 2
    mats = [(wa_s, 0, half, [wk_ref, wv_ref]), (wqf_s, 0, half, [wq_ref])]
    mq, mo = 1, 2

    def share(v):
        return lax.div(v, dp // 2), lax.rem(v, dp // 2)

    def wide(mat):
        return 2 * mats[mat][2] // dp

    def piece(mat, o, v):
        r, b = share(v)
        if mat < mo:
            ref, col, _, _ = mats[mat]
            return ref.at[pl.ds(pl.multiple_of((2 * o + r) * rows, 16), rows), pl.ds(pl.multiple_of(col + b * wide(mat), 128), wide(mat))]
        return wof_s.at[pl.ds(pl.multiple_of((2 * o + k) * rows_o + b * hi, 16), hi), pl.ds(pl.multiple_of(r * ho, 128), ho)]

    def several(mat, count):
        ref, h, w = (mats[mat][0], n * 2 * rows, mats[mat][2]) if mat < mo else (wof_s, n * rows_o, d)
        if h * count % (dp * n) == 0 and h * count // (dp * n) % 16 == 0:
            return ref.at[pl.ds(0, h * count // (dp * n)), pl.ds(0, w)]
        tall, broad = (rows, wide(mat)) if mat < mo else (hi, ho)
        return ref.at[pl.ds(0, tall * count), pl.ds(0, broad)]

    r, b = share(g)

    def sources(mat, kk):
        _, _, cols, refs = mats[mat]
        each = cols // len(refs)
        at = b * wide(mat)
        for i, ref in enumerate(refs):
            cond = None if len(refs) == 1 else lax.div(at, each) == i
            yield cond, ref.at[:, pl.ds(pl.multiple_of(kk * each + lax.rem(at, each), 128), wide(mat))]

    def maybe(cond, f):
        f() if cond is None else pl.when(cond)(f)

    def begin_here(mat):
        if mat == mo:
            src = wo_ref.at[pl.ds(pl.multiple_of(b * hi, 16), hi), pl.ds(pl.multiple_of(r * ho, 128), ho)]
            pltpu.make_async_copy(src, piece(mo, c, g), pre_sem.at[mo]).start()
            return

        @pl.when(k == r)
        def _():
            for cond, src in sources(mat, k):
                maybe(cond, lambda: pltpu.make_async_copy(src, piece(mat, c, g), pre_sem.at[mat]).start())

    def begin_there(mat):
        @pl.when(k == r)
        def _():
            for cond, src in sources(mat, 1 - k):
                maybe(cond, lambda: remote(src, piece(mat, c, g), pre_send.at[mat], pre_sem.at[mat], sib).start())

    def hop(mat, o, way, step):
        remote(piece(mat, o, g), piece(mat, o, g), zs_sem.at[mat], zr_sem.at[mat, way, step], (right, left)[way]).start()

    def across(mat, o):
        first = lax.rem(o, 2)
        for p in range(1, m):
            near, far = jnp.where(first == 0, row(p), column(p)), jnp.where(first == 0, column(p), row(p))
            remote(piece(mat, o, g), piece(mat, o, g), xys_sem.at[mat], near_sem.at[mat, o], (near, me)).start()
            remote(piece(mat, o, g), piece(mat, o, g), xys_sem.at[mat], far_sem.at[mat], (far, me)).start()

    def hand_on(mat, o):
        first = lax.rem(o, 2)
        await_(several(mat, m - 1), near_sem.at[mat, o])
        for q in range(1, m):
            for p in range(1, m):
                v, far = jnp.where(first == 0, row(q), column(q)), jnp.where(first == 0, column(p), row(p))
                remote(piece(mat, o, v), piece(mat, o, v), xys_sem.at[mat], far_sem.at[mat], (far, me)).start()

    def for_chips(f, mat):
        lax.fori_loop(0, n, lambda o, _: f(mat, o), None)

    def arrived(mat):
        await_(several(mat, n * m * (m - 1)), far_sem.at[mat])

    def reach(mat):
        return (down, up) if mat == mq else (up, down)

    def ring(mat, s, f=None):
        for way, last in enumerate(reach(mat)):
            if s <= last:
                o = lax.rem(c + n - s, n) if way == 0 else lax.rem(c + s, n)
                await_(piece(mat, o, g), zr_sem.at[mat, way, s - 1])
                if s < last:
                    hop(mat, o, way, s)
                if f is not None:
                    f(mat, o)

    def set_out(mat):
        await_(piece(mat, c, g), pre_sem.at[mat])
        for way, last in enumerate(reach(mat)):
            if last:
                hop(mat, c, way, 0)

    gain = gain_ref[...].astype(F32).reshape(1, d)
    tile = 32

    def norm(src, at, to):
        wide_x = src[pl.ds(at, tile), :].astype(F32)
        scale = lax.rsqrt(jnp.mean(wide_x * wide_x, -1, keepdims=True) + 1e-6)
        a_s[pl.ds(to, tile), :] = (wide_x * scale * gain).astype(BF16)

    def norm_own(i, _):
        norm(xr_s, _at(i, tile), pl.multiple_of(k * own + i * tile, tile))

    def norm_other(i, _):
        at = pl.multiple_of((1 - k) * own + i * tile, tile)
        norm(a_s, at, at)

    def angles(i, _):
        at = pl.ds(_at(i, 64), 64)
        place = c * tokens + i * 64 + lax.broadcasted_iota(jnp.int32, (64, HEAD // 2), 0)
        angle = place.astype(F32) * freq_ref[...]
        cos_s[at, :] = jnp.cos(angle)
        sin_s[at, :] = jnp.sin(angle)

    steps = own // tile
    for mat in range(3):
        begin_here(mat)
    x_in = pltpu.make_async_copy(x_ref, xr_s, x_sem.at[0])
    x_in.start()
    pl.semaphore_wait(barrier, 3 + 2 * (m - 1))
    begin_there(0)
    begin_there(1)
    x_out = remote(x_ref, a_s.at[pl.ds(pl.multiple_of(k * own, own), own), :], x_sem.at[1], x_sem.at[2], sib)
    x_out.start()
    set_out(0)
    across(0, c)
    set_out(1)
    x_in.wait()
    lax.fori_loop(0, steps, norm_own, None)

    def both(step):
        if step == 0:
            return [c]
        return [lax.rem(c + n - step, n)] * (step <= up) + [lax.rem(c + step, n)] * (step <= down)

    def hand_on_all(step):
        for o in both(step):
            hand_on(0, o)

    tiles, spread = tokens // 64, max(up - 1, 1)
    for s in range(1, up + 1):
        ring(0, s, across)
        if s == 1:
            set_out(mo)
        elif s == 2:
            ring(mq, 1)
        elif s == 3:
            ring(mo, 1)
        else:
            ring(mq, s - 2)
            ring(mo, s - 2)
        hand_on_all(s - 1)
        if s == 1:
            await_(a_s.at[pl.ds(pl.multiple_of((1 - k) * own, own), own), :], x_sem.at[2])
            lax.fori_loop(0, steps, norm_other, None)
        if s > 1 or up == 1:
            lax.fori_loop((s - 2) * tiles // spread if up > 1 else 0, (s - 1) * tiles // spread if up > 1 else tiles, angles, None)
    rest = [(mat, s) for s in range(1, up + 1) for mat in (mq, mo) if not (s <= up - 2 or (s == 1 and up >= (2 if mat == mq else 3)))]
    handed = False
    for mat, s in rest[:-1]:
        ring(mat, s)
        if not handed:
            hand_on_all(up)
            handed = True
    if not handed:
        hand_on_all(up)
    for i in range(KVH):
        top_s[i] = jnp.full((1, GROUP * tokens), NEG, F32)
        mix_s[i] = jnp.zeros((HEAD + 8, GROUP * tokens), F32)

    def project(w_ref, col, t, turn):
        at = pl.ds(_at(t, BK), BK)
        out = jnp.dot(a_s[at, :], w_ref[:, pl.ds(pl.multiple_of(col, HEAD), HEAD)], preferred_element_type=F32).astype(BF16)
        if turn:
            cos, sin = cos_s[at, :], sin_s[at, :]
            lo, up_ = out[:, : HEAD // 2].astype(F32), out[:, HEAD // 2 :].astype(F32)
            out = jnp.concatenate([lo * cos - up_ * sin, up_ * cos + lo * sin], -1).astype(BF16)
        return out

    def pass_on(o, way, p, step):
        remote(kv_s.at[o, way, p], kv_s.at[o, way, p], ks_sem.at[way], kr_sem.at[way, p, step], (right, left)[way]).start()

    parts = tokens // BK
    pieces = 2 * parts

    def own_keys(t, _):
        for p in range(2):
            def one(i, _):
                kv_s[c, i, 2 * t + p] = project(wa_s, (p * KVH + i) * HEAD, t, p == 0)

            lax.fori_loop(0, KVH, one, None)
            for i in range(KVH):
                pass_on(c, i, 2 * t + p, 0)

    arrived(0)
    for_chips(across, mq)
    lax.fori_loop(0, parts, own_keys, None)
    for mat, s in rest[-1:]:
        ring(mat, s)

    def queries():
        def one(h, _):
            def some(t, _):
                at = pl.ds(pl.multiple_of(lax.rem(h, GROUP) * tokens + t * BK, BK), BK)
                q_s[lax.div(h, GROUP), at, :] = project(wqf_s, h * HEAD, t, True)

            lax.fori_loop(0, tokens // BK, some, None)

        lax.fori_loop(0, KVH * GROUP, one, None)

    e = HEAD**-0.5 * LOG2E
    ones = jnp.ones((8, BK), BF16)

    def block(i, o, j, strips, masked):
        kk = kv_s[o, i, 2 * j]
        scores = [_dot(kk, q_s[i, at : at + STRIP, :], 1, 1) for at in strips]
        weights, keeps = [], []
        for at, s in zip(strips, scores):
            if masked and at % tokens < (j + 1) * BK - 1:
                gap = lax.broadcasted_iota(jnp.int32, (BK, STRIP), 1) - lax.broadcasted_iota(jnp.int32, (BK, STRIP), 0)
                s = jnp.where(gap >= j * BK - at % tokens, s, HIDDEN)
            old = top_s[i, :, at : at + STRIP]
            top = jnp.maximum(old, s.max(axis=0, keepdims=True))
            top_s[i, :, at : at + STRIP] = top
            weights.append(jnp.exp2((s - top) * e).astype(BF16))
            keeps.append(jnp.exp2((old - top) * e))
        values = jnp.concatenate([kv_s[o, i, 2 * j + 1].T, ones], axis=0)
        for at, p, keep in zip(strips, weights, keeps):
            mix_s[i, :, at : at + STRIP] = mix_s[i, :, at : at + STRIP] * keep + _dot(values, p, 1, 0)

    every = list(range(0, GROUP * tokens, STRIP))

    def own_chunk():
        def one(i, _):
            for j in range(parts):
                block(i, c, j, [at for at in every if at % tokens + STRIP > j * BK], True)

        lax.fori_loop(0, KVH, one, None)

    def origin(way, s):
        return lax.rem(jnp.where(way == 0, c + n - s, c + s), n)

    def unit(u, _):
        s, j = lax.div(u, parts) + 1, lax.rem(u, parts)

        def one(i, _):
            @pl.when(origin(i, s) < c)
            def _():
                block(i, origin(i, s), j, every, False)

        lax.fori_loop(0, KVH, one, None)

    def left_sent(mat):
        await_(several(mat, n * (dp - 1)), xys_sem.at[mat])
        if up:
            await_(several(mat, up + down), zs_sem.at[mat])

    def spot(x):
        return slice(x // 2 * BK, x // 2 * BK + BK), slice(x % 2 * STRIP, x % 2 * STRIP + STRIP)

    def last_weights():
        for mat in range(2):
            left_sent(mat)
        for i in range(KVH):
            o = origin(i, n - 1)

            @pl.when(o < c)
            def _():
                kk = kv_s[o, i, 2 * (parts - 1)]
                scores = [_dot(kk, q_s[i, at : at + STRIP, :], 1, 1) for at in every]
                for x, (at, s) in enumerate(zip(every, scores)):
                    old = top_s[i, :, at : at + STRIP]
                    top = jnp.maximum(old, s.max(axis=0, keepdims=True))
                    top_s[i, :, at : at + STRIP] = top
                    (wa_s, wqf_s)[i][spot(x)] = jnp.exp2((s - top) * e).astype(BF16)
                    keep_s[i, :, at : at + STRIP] = jnp.exp2((old - top) * e)

    def last_values():
        for i in range(KVH):
            o = origin(i, n - 1)

            @pl.when(o < c)
            def _():
                values = jnp.concatenate([kv_s[o, i, 2 * parts - 1].T, ones], axis=0)
                for x, at in enumerate(every):
                    kept = mix_s[i, :, at : at + STRIP] * keep_s[i, :, at : at + STRIP]
                    mix_s[i, :, at : at + STRIP] = kept + _dot(values, (wa_s, wqf_s)[i][spot(x)], 1, 0)

    def share_wo():
        arrived(mo)

        def send(o, _):
            at = pl.ds(pl.multiple_of((2 * o + k) * rows_o, 16), rows_o)
            remote(wof_s.at[at, :], wof_s.at[at, :], wo_sem.at[0], wo_sem.at[1], sib).start()

        lax.fori_loop(0, n, send, None)

    def take(q):
        s, p = lax.div(q, pieces) + 1, lax.rem(q, pieces)
        for way in range(2):
            o = origin(way, s)
            await_(kv_s.at[o, way, p], kr_sem.at[way, p, s - 1])

            @pl.when(s < n - 1)
            def _():
                pass_on(o, way, p, s)

    end = pieces * (n - 1)
    at_wq, at_q, at_own, at_wo, at_share = (min(i, end - 1) for i in (2, 5, 6, 9, 14))

    def main(q, done):
        take(q)

        @pl.when(q == at_wq)
        def _():
            for_chips(hand_on, mq)

        @pl.when(q == at_q)
        def _():
            arrived(mq)
            for_chips(across, mo)
            queries()

        @pl.when(q == at_own)
        def _():
            own_chunk()

        @pl.when(q == at_wo)
        def _():
            for_chips(hand_on, mo)

        @pl.when(q == at_share)
        def _():
            share_wo()

        until = jnp.where(q > at_own, jnp.minimum(done + 2, jnp.minimum(lax.div(q + 1, 2), end // 2 - 1)), 0)
        lax.fori_loop(done, until, unit, None)

        @pl.when(q == end - 2)
        def _():
            last_weights()

        return until

    lax.fori_loop(0, end, main, jnp.int32(0))
    last_values()

    def result(j, at):
        i, h = lax.div(j, GROUP), lax.rem(j, GROUP)
        cols = pl.ds(pl.multiple_of(h * tokens + at, own), own)
        return (mix_s[i, :HEAD, cols] * (1 / mix_s[i, HEAD : HEAD + 1, cols])).T.astype(BF16)

    def theirs(j, _):
        os_s[j] = result(j, (1 - k) * own)

    def ours(j, _):
        o_s[k, j] = result(j, k * own)

    heads = KVH * GROUP
    lax.fori_loop(0, heads, theirs, None)
    o_out = remote(os_s, o_s.at[k], o_sem.at[0], o_sem.at[1], sib)
    o_out.start()
    lax.fori_loop(0, heads, ours, None)
    whole = wof_s.at[pl.ds(0, n * rows_o), :]
    await_(whole, wo_sem.at[1])
    hw, col, kept = heads * HEAD, 256, GROUP * tokens // 256

    def product(kk, at):
        seen = jnp.concatenate([o_s[kk, h] for h in range(heads)], axis=1)
        return jnp.dot(seen, wof_s[pl.ds(pl.multiple_of(kk * hw, hw), hw), at], preferred_element_type=F32)

    def half_done(j, _):
        at = pl.ds(_at(j, col), col)
        out = product(k, at)
        for i in range(2):
            mix_s[i, : own // 2, at] = out[i * own // 2 : (i + 1) * own // 2]

    lax.fori_loop(0, min(kept, d // col), half_done, None)
    await_(o_s.at[1 - k], o_sem.at[1])

    def finish(j, _):
        at = pl.ds(_at(j, col), col)
        out = product(1 - k, at)
        for i in range(2):
            part = slice(i * own // 2, (i + 1) * own // 2)
            y_ref[part, at] = (xr_s[part, at].astype(F32) + (mix_s[i, : own // 2, at] + out[part])).astype(BF16)

    lax.fori_loop(0, min(kept, d // col), finish, None)
    for j in range(kept, d // col):
        at = pl.ds(j * col, col)
        y_ref[:, at] = (xr_s[:, at].astype(F32) + (product(k, at) + product(1 - k, at))).astype(BF16)

    o_out.wait_send()
    x_out.wait_send()
    await_(whole, wo_sem.at[0])
    left_sent(mo)

    @pl.when(k == r)
    def _():
        for mat in range(mo):
            await_(piece(mat, c, g), pre_send.at[mat])

    for way in range(2):
        await_(kv_s.at[pl.ds(0, n - 1), way], ks_sem.at[way])


def solution(mesh):
    dp, sp = mesh.shape["dp"], mesh.shape["sp"]

    def step(x, gain, wq, wk, wv, wo):
        own, d = x.shape
        n = sp // 2
        tokens = 2 * own
        half_d = wq.shape[1] // 2
        up, down = n // 2, (n - 1) // 2
        hh = HEAD // 2
        freq = (THETA ** (-np.arange(hh, dtype=np.float32) / hh)).astype(np.float32)[None]
        vm, any_ = pl.BlockSpec(memory_space=pltpu.VMEM), pl.BlockSpec(memory_space=pl.ANY)
        dma = pltpu.SemaphoreType.DMA
        return pl.pallas_call(
            functools.partial(kernel, dp, sp),
            out_shape=pltpu.VMEM((own, d), BF16),
            in_specs=[any_, vm, vm, any_, any_, any_, any_],
            out_specs=vm,
            scratch_shapes=[
                pltpu.VMEM((tokens, d), BF16),
                pltpu.VMEM((own, d), BF16),
                pltpu.VMEM((tokens, hh), F32),
                pltpu.VMEM((tokens, hh), F32),
                pltpu.VMEM((d, half_d), BF16),
                pltpu.VMEM((d, half_d), BF16),
                pltpu.VMEM((2 * half_d, d), BF16),
                pltpu.VMEM((n, KVH, 2 * tokens // BK, BK, HEAD), BF16),
                pltpu.VMEM((KVH, GROUP * tokens, HEAD), BF16),
                pltpu.VMEM((KVH, 1, GROUP * tokens), F32),
                pltpu.VMEM((KVH, 1, GROUP * tokens), F32),
                pltpu.VMEM((KVH, HEAD + 8, GROUP * tokens), F32),
                pltpu.VMEM((2, KVH * GROUP, own, HEAD), BF16),
                pltpu.VMEM((KVH * GROUP, own, HEAD), BF16),
                dma((3,)), dma((3,)), dma((2,)), dma((3, 2, max(up, 1))), dma((3,)), dma((3, n)), dma((3,)), dma((3,)),
                dma((2, 2 * tokens // BK, max(n - 1, 1))), dma((2,)), dma((2,)), dma((2,)),
            ],
            compiler_params=pltpu.CompilerParams(collective_id=0, has_side_effects=True, vmem_limit_bytes=62 * 10**6),
        )(x, gain, freq, wq, wk, wv, wo)

    tokens, whole = P(("dp", "sp"), None), P("sp", None)
    return jax.shard_map(
        step,
        mesh=mesh,
        in_specs=(tokens, P(None), whole, whole, whole, whole),
        out_specs=tokens,
        check_vma=False,
    )
```
